8 devices in a mesh: rep: 2 (over y, z), dp: 4 (over x, core).
Axes of the slice: x: 2, y: 2, z: 1, core: 2. Of those that a mesh axis runs over, the one named last changes fastest.
Arguments:
- x: bfloat16 [8, 2048, 512], P(('rep', 'dp')), parts along dimension 0
- dy: bfloat16 [8, 2048, 512], P(('rep', 'dp')), parts along dimension 0
- w_gate: bfloat16 [2, 512, 4096], P(None, 'dp')
- w_up: bfloat16 [2, 512, 4096], P(None, 'dp')
- w_down: bfloat16 [2, 4096, 512], P(None, 'dp')
Outputs:
- output 1: bfloat16 [8, 2048, 512], P(('rep', 'dp')), parts along dimension 0
- output 2: bfloat16 [4, 512, 4096], P('rep', 'dp'), parts along dimension 0
- output 3: bfloat16 [4, 512, 4096], P('rep', 'dp'), parts along dimension 0
- output 4: bfloat16 [4, 4096, 512], P('rep', 'dp'), parts along dimension 0
There are 2 independent parts. The reference program is written for one: setup_inputs(seed, part) draws one part's arguments, and reference() takes and returns one part's arrays. A program takes and returns all parts, laid end to end along the dimension named above; an argument that names none is the same for every part.
All inputs are finite; a program needn't handle non-finite values.
Results may differ from the reference program's by a relative error of at most 0.018.
Values are sent between devices in bfloat16 or wider.
A program may use at most 2 GiB of HBM per device.

```python
import jax
import jax.numpy as jnp
from jax import lax

SEQUENCES = 4
TOKENS = 2048
D = 512
FF = 4096
LAYERS = 2
NAMES = ("w_gate", "w_up", "w_down")
SHAPES = {"w_gate": (LAYERS, D, FF), "w_up": (LAYERS, D, FF), "w_down": (LAYERS, FF, D)}


def bump(key, n, height):
    away = (jnp.arange(n, dtype=jnp.int32) - jax.random.randint(key, (), 0, n, jnp.int32)) % n
    return jnp.where(away < n // 8, height, 1.0)


def together(key, own, strength):
    shared = jax.random.normal(key, own.shape[1:], jnp.float32)
    return (own + strength * shared) * lax.rsqrt(1 + strength * strength)


def setup_inputs(seed: int = 0, part: int = 0) -> dict:
    kx, kdy, ka, kb, kz, kf, kh, kl, *kw = jax.random.split(jax.random.key(seed), 8 + len(NAMES))
    kx, kdy, ka, kb = (jax.random.fold_in(k, part) for k in (kx, kdy, ka, kb))
    shape = (SEQUENCES, TOKENS, D)
    much_x, much_dy = jax.random.uniform(kz, (2,), jnp.float32, 0.0, 1.0)
    layers = 2.0 ** jax.random.uniform(kl, (LAYERS, 1, 1), jnp.float32, -1.0, 1.0)
    x = together(ka, jax.random.normal(kx, shape, jnp.float32), much_x) * bump(kf, D, 4.0)
    dy = together(kb, jax.random.normal(kdy, shape, jnp.float32), much_dy)
    drawn = {"x": x.astype(jnp.bfloat16), "dy": (dy * (SEQUENCES * TOKENS) ** -0.5).astype(jnp.bfloat16)}
    for key, name in zip(kw, NAMES, strict=True):
        w = jax.random.normal(key, SHAPES[name], jnp.float32) * SHAPES[name][1] ** -0.5
        drawn[name] = (w * {"w_gate": 1.0, "w_up": bump(kh, FF, 4.0), "w_down": layers}[name]).astype(jnp.bfloat16)
    return drawn


def matmul(a, w):
    return jnp.dot(a, w, preferred_element_type=jnp.float32).astype(jnp.bfloat16)


def normed(h):
    wide = h.astype(jnp.float32)
    scale = lax.rsqrt(jnp.mean(wide**2, -1, keepdims=True) + 1e-6)
    return (wide * scale).astype(jnp.bfloat16)


def layer(h, w):
    a = normed(h)
    gate = jnp.dot(a, w["w_gate"], preferred_element_type=jnp.float32)
    up = jnp.dot(a, w["w_up"], preferred_element_type=jnp.float32)
    return h + matmul((jax.nn.silu(gate) * up).astype(jnp.bfloat16), w["w_down"])


def stack(weights, h):
    return lax.scan(lambda h, w: (layer(h, w), None), h, weights)[0]


def reference(x, dy, w_gate, w_up, w_down):
    weights = dict(zip(NAMES, (w_gate, w_up, w_down), strict=True))

    def take(so_far, sequence):
        h, by_y = sequence
        _, back = jax.vjp(stack, weights, h)
        by_weights, by_h = back(by_y)
        return jax.tree.map(lambda total, term: total + term.astype(jnp.float32), so_far, by_weights), by_h

    none_yet = {name: jnp.zeros(w.shape, jnp.float32) for name, w in weights.items()}
    by_weights, by_x = lax.scan(take, none_yet, (x, dy))
    return (by_x, *(by_weights[name].astype(jnp.bfloat16) for name in NAMES))
```

```python
import jax
import jax.numpy as jnp
from jax import lax
from jax.experimental import pallas as pl
from jax.experimental.pallas import tpu as pltpu
from jax.sharding import PartitionSpec as P

f32, bf16 = jnp.float32, jnp.bfloat16
MESH = pl.DeviceIdType.MESH
TT, D, FF, LAYERS = 2048, 512, 4096, 2
FB = 512
NF = FF // FB
UNITS = LAYERS * NF
SLAB = 128
T = 1024
NT = TT // T
TN = 256


def dot(a, b):
    return lax.dot_general(a, b, (((1,), (0,)), ((), ())), preferred_element_type=f32)


def dot_nt(a, b):
    return lax.dot_general(a, b, (((1,), (1,)), ((), ())), preferred_element_type=f32)


def sigmoid(g):
    return 0.5 * jnp.tanh(0.5 * g) + 0.5


def tile(i, size):
    return pl.ds(pl.multiple_of(i * size, size), size)


def rms(wide):
    return lax.rsqrt(jnp.mean(wide * wide, -1, keepdims=True) + 1e-6)


def kernel(
    x_in, dy_in, wg_in, wu_in, wd_in,
    bx_out, dwg_out, dwu_out, dwd_out, WH, RDH, RXH,
    OWN, W, X, A, AT, DY, DYT, H1, ACC, PB, GB, UB, DWB, KEEP, OACC, SD, SX, RDV, RXV, OUTB,
    s_own, s_ownh, s_p, r_p, s_x, r_x, s_y, r_y, s_f, r_f, s_w, s_sd, r_rd, s_rdv, s_sx, r_rx, s_rxv, s_out, s_act,
):
    r, me = lax.axis_index("rep"), lax.axis_index("dp")
    chip, core = me // 2, me % 2
    partner = {"rep": r, "dp": chip * 2 + 1 - core}
    xnbr = {"rep": r, "dp": (1 - chip) * 2 + core}
    ynbr = {"rep": 1 - r, "dp": me}
    far = (1 - chip) * 2 + core

    def rows(d):
        return pl.ds(pl.multiple_of(d * SLAB, SLAB), SLAB)

    def remote(src, dst, send, recv, dev):
        return pltpu.make_async_remote_copy(src_ref=src, dst_ref=dst, send_sem=send, recv_sem=recv, device_id=dev, device_id_type=MESH)

    def order(j):
        return (1 - j // NF) * NF + 2 * ((j % NF) // 2) + lax.rem(r + j, 2)

    def own_loads(u):
        l, f = u // NF, u % NF
        for m, w in enumerate((wg_in, wu_in)):
            for s in range(4):
                yield pltpu.make_async_copy(
                    w.at[l, :, pl.ds(pl.multiple_of(s * 1024 + f * SLAB, SLAB), SLAB)],
                    OWN.at[u, m, :, pl.ds(s * SLAB, SLAB)], s_own.at[u])
        yield pltpu.make_async_copy(wd_in.at[l, tile(f, SLAB), :], OWN.at[u, 2], s_own.at[u])

    def own_home(u):
        return pltpu.make_async_copy(OWN.at[u], WH.at[u, :, rows(me), :], s_ownh.at[u])

    def own_partner(u):
        return remote(OWN.at[u], WH.at[u, :, rows(me), :], s_p.at[u], r_p.at[u], partner)

    def own_x(k):
        u = 2 * k + r
        return remote(OWN.at[u], WH.at[u, :, rows(me), :], s_x.at[k], r_x.at[k], xnbr)

    def forward_y(k):
        u = 2 * k + r
        here = WH.at[u, :, rows(far), :]
        return remote(here, here, s_y.at[k], r_y.at[k], ynbr)

    def forward_partner(u):
        here = WH.at[u, :, rows(far), :]
        return remote(here, here, s_f.at[u], r_f.at[u], partner)

    def arrived_x(k):
        own_x(k).wait_recv()
        forward_y(k).start()
        forward_partner(2 * k + r).start()

    def arrived_y(k):
        forward_y(k).wait_recv()
        forward_partner(2 * k + 1 - r).start()

    def load_w(u, slot):
        return pltpu.make_async_copy(WH.at[u], W.at[slot], s_w.at[slot])

    def fetch_w(u, slot):
        own_partner(u).wait_recv()
        forward_partner(u).wait_recv()
        load_w(u, slot).start()

    def send_terms(u, slot):
        return remote(SD.at[slot], RDH.at[u], s_sd.at[slot], r_rd.at[u], partner)

    def load_terms(u):
        return pltpu.make_async_copy(RDH.at[u], RDV, s_rdv)

    def send_sum(u, slot):
        return remote(SX.at[slot], RXH.at[u], s_sx.at[slot], r_rx.at[u], xnbr)

    def load_sum(u):
        return pltpu.make_async_copy(RXH.at[u], RXV, s_rxv)

    def store_outs(u, slot):
        l, f = u // NF, u % NF
        for m, w in enumerate((dwg_out, dwu_out)):
            for s in range(4):
                yield pltpu.make_async_copy(
                    OUTB.at[slot, m, :, pl.ds(s * SLAB, SLAB)],
                    w.at[l, :, pl.ds(pl.multiple_of(s * 1024 + f * SLAB, SLAB), SLAB)], s_out.at[slot])
        yield pltpu.make_async_copy(OUTB.at[slot, 2], dwd_out.at[l, tile(f, SLAB), :], s_out.at[slot])

    def wait_outs(slot):
        pltpu.make_async_copy(OUTB.at[slot], RXH.at[0], s_out.at[slot]).wait()

    barrier = pltpu.get_barrier_semaphore()
    for dev in (partner, xnbr, ynbr):
        pl.semaphore_signal(barrier, inc=1, device_id=dev, device_id_type=MESH)

    @pl.loop(0, UNITS)
    def _(u):
        for c in own_loads(u):
            c.start()

    load_x = pltpu.make_async_copy(x_in.at[0], X, s_act.at[0])
    load_dy = pltpu.make_async_copy(dy_in.at[0], DY, s_act.at[1])
    load_x.start()
    load_dy.start()
    pl.semaphore_wait(barrier, 3)

    @pl.loop(0, UNITS // 2)
    def _(k):
        for q in (r, 1 - r):
            u = 2 * k + q
            pltpu.make_async_copy(RXH.at[0], OWN.at[u], s_own.at[u]).wait()
            own_partner(u).start()
            own_home(u).start()
        own_x(k).start()

    load_x.wait()
    load_dy.wait()

    @pl.loop(0, TT // TN)
    def _(t):
        tt = tile(t, TN)
        wide = X[tt, :].astype(f32)
        A[tt, :] = (wide * rms(wide)).astype(bf16)
        DYT[:, tt] = DY[tt, :].T
        ACC[tt, :] = jnp.zeros((TN, D), f32)

    @pl.loop(0, UNITS)
    def _(u):
        own_home(u).wait()

    @pl.loop(0, NF // 2 + 1)
    def _(k):
        arrived_x(k)

        @pl.when(k >= 1)
        def _():
            arrived_y(k - 1)

        @pl.when(k < NF // 2)
        def _():
            fetch_w(2 * k + r, 0)

        @pl.when(k >= 1)
        def _():
            fetch_w(2 * (k - 1) + 1 - r, 1)

        first, last = jnp.where(k < NF // 2, 0, 1), jnp.where(k >= 1, 2, 1)

        @pl.loop(first, last)
        def _(slot):
            load_w(0, slot).wait()

            @pl.loop(0, NT)
            def _(t):
                tt = tile(t, T)
                a = A[tt, :]
                g = dot(a, W[slot, 0])
                up = dot(a, W[slot, 1])
                p = (g * sigmoid(g) * up).astype(bf16)
                ACC[tt, :] += dot(p, W[slot, 2])

    fetch_w(order(0), 0)

    @pl.loop(0, TT // TN)
    def _(t):
        tt = tile(t, TN)
        h = (X[tt, :].astype(f32) + ACC[tt, :].astype(bf16).astype(f32)).astype(bf16)
        H1[tt, :] = h
        wide = h.astype(f32)
        a = (wide * rms(wide)).astype(bf16)
        A[tt, :] = a
        AT[:, tt] = a.T
        ACC[tt, :] = jnp.zeros((TN, D), f32)

    def sum_terms(j):
        slot = j % 2

        @pl.when(j >= 2)
        def _():
            send_sum(0, slot).wait_send()

        for m in range(3):
            OACC[j % 4, m] = KEEP[0, m] + RDV[0, m].astype(f32)
            SX[slot, m] = (KEEP[1, m] + RDV[1, m].astype(f32)).astype(bf16)
        send_sum(order(j), slot).start()

    def finish(j):
        slot = j % 2

        @pl.when(j >= 2)
        def _():
            wait_outs(slot)

        for m in range(3):
            OUTB[slot, m] = (OACC[j % 4, m] + RXV[m].astype(f32)).astype(bf16)
        for c in store_outs(order(j), slot):
            c.start()

    def ask_terms(j):
        send_terms(order(j), 0).wait_recv()
        load_terms(order(j)).start()

    def ask_sum(j):
        send_sum(order(j), 0).wait_recv()
        load_sum(order(j)).start()

    def backward_unit(j):
        slot = j % 2
        load_w(0, slot).wait()

        @pl.loop(0, NT)
        def _(t):
            tt = tile(t, T)
            a = A[tt, :]
            g = dot(a, W[slot, 0])
            up = dot(a, W[slot, 1])
            dp = dot_nt(DY[tt, :], W[slot, 2]).astype(bf16).astype(f32)
            sig = sigmoid(g)
            s = g * sig
            PB[tt, :] = (s * up).astype(bf16)
            du = (dp * s).astype(bf16)
            dg = (dp * up * (sig + s * (1 - sig))).astype(bf16)
            UB[tt, :] = du
            GB[tt, :] = dg
            ACC[tt, :] += dot_nt(dg, W[slot, 0]) + dot_nt(du, W[slot, 1])

            @pl.when((t == 0) & (j >= 1))
            def _():
                ask_terms(j - 1)

            @pl.when((t == 0) & (j >= 3))
            def _():
                ask_sum(j - 3)

        @pl.when(j >= 1)
        def _():
            load_terms(0).wait()
            sum_terms(j - 1)

        @pl.when(j >= 3)
        def _():
            load_sum(0).wait()
            finish(j - 3)

        @pl.when(j >= 2)
        def _():
            send_terms(0, slot).wait_send()

        for m in range(3):
            if m == 0:
                term = dot(AT[...], GB[...])
            elif m == 1:
                term = dot(AT[...], UB[...])
            else:
                term = dot(DYT[...], PB[...]).T
            DWB[...] = term
            KEEP[0, m] = DWB[rows(me), :]
            KEEP[1, m] = DWB[rows(far), :]
            SD[slot, 0, m] = DWB[rows(partner["dp"]), :].astype(bf16)
            SD[slot, 1, m] = DWB[rows((1 - chip) * 2 + 1 - core), :].astype(bf16)
        send_terms(order(j), slot).start()

    def norm_back(h, t):
        wide = h.astype(f32)
        scale = rms(wide)
        da = ACC[tile(t, TN), :].astype(bf16).astype(f32)
        along = jnp.sum(da * wide, -1, keepdims=True) * (scale * scale * scale) * (1.0 / D)
        back = (da * scale - wide * along).astype(bf16)
        return (DY[tile(t, TN), :].astype(f32) + back.astype(f32)).astype(bf16)

    @pl.loop(0, NF)
    def _(j):
        @pl.when(j < 3)
        def _():
            arrived_x(j + 5)

        @pl.when(j < 4)
        def _():
            arrived_y(j + 4)

        backward_unit(j)

        @pl.when(j < NF - 1)
        def _():
            fetch_w(order(j + 1), (j + 1) % 2)

    load_w(order(NF), 0).start()

    @pl.loop(0, TT // TN)
    def _(t):
        tt = tile(t, TN)
        dh = norm_back(H1[tt, :], t)
        DY[tt, :] = dh
        DYT[:, tt] = dh.T
        wide = X[tt, :].astype(f32)
        a = (wide * rms(wide)).astype(bf16)
        A[tt, :] = a
        AT[:, tt] = a.T
        ACC[tt, :] = jnp.zeros((TN, D), f32)

    @pl.loop(NF, UNITS)
    def _(j):
        @pl.when(j < UNITS - 1)
        def _():
            load_w(order(j + 1), (j + 1) % 2).start()

        backward_unit(j)

    @pl.loop(0, TT // TN)
    def _(t):
        tt = tile(t, TN)
        H1[tt, :] = norm_back(X[tt, :], t)

    store_x = pltpu.make_async_copy(H1, bx_out.at[0], s_act.at[0])
    store_x.start()

    last = UNITS - 1
    ask_terms(last)
    load_terms(0).wait()
    sum_terms(last)
    for j in (last - 2, last - 1, last):
        ask_sum(j)
        load_sum(0).wait()
        finish(j)

    store_x.wait()
    for slot in range(2):
        wait_outs(slot)
        send_terms(0, slot).wait_send()
        send_sum(0, slot).wait_send()

    @pl.loop(0, UNITS // 2)
    def _(k):
        own_x(k).wait_send()
        forward_y(k).wait_send()

    @pl.loop(0, UNITS)
    def _(u):
        own_partner(u).wait_send()
        forward_partner(u).wait_send()


def solution(mesh):
    def step(x, dy, w_gate, w_up, w_down):
        vmem, dma = pltpu.VMEM, pltpu.SemaphoreType.DMA
        hbm = pl.BlockSpec(memory_space=pl.ANY)
        shape = jax.ShapeDtypeStruct
        outs = pl.pallas_call(
            kernel,
            out_shape=(
                shape(x.shape, bf16), shape(w_gate.shape, bf16), shape(w_up.shape, bf16), shape(w_down.shape, bf16),
                shape((UNITS, 3, D, FB), bf16), shape((UNITS, 2, 3, SLAB, FB), bf16), shape((UNITS, 3, SLAB, FB), bf16),
            ),
            in_specs=[hbm] * 5,
            out_specs=[hbm] * 7,
            scratch_shapes=[
                vmem((UNITS, 3, SLAB, FB), bf16),
                vmem((2, 3, D, FB), bf16),
                vmem((TT, D), bf16),
                vmem((TT, D), bf16),
                vmem((D, TT), bf16),
                vmem((TT, D), bf16),
                vmem((D, TT), bf16),
                vmem((TT, D), bf16),
                vmem((TT, D), f32),
                vmem((TT, FB), bf16),
                vmem((TT, FB), bf16),
                vmem((TT, FB), bf16),
                vmem((D, FB), f32),
                vmem((2, 3, SLAB, FB), f32),
                vmem((4, 3, SLAB, FB), f32),
                vmem((2, 2, 3, SLAB, FB), bf16),
                vmem((2, 3, SLAB, FB), bf16),
                vmem((2, 3, SLAB, FB), bf16),
                vmem((3, SLAB, FB), bf16),
                vmem((2, 3, SLAB, FB), bf16),
                dma((UNITS,)), dma((UNITS,)),
                dma((UNITS,)), dma((UNITS,)),
                dma((UNITS // 2,)), dma((UNITS // 2,)),
                dma((UNITS // 2,)), dma((UNITS // 2,)),
                dma((UNITS,)), dma((UNITS,)),
                dma((2,)),
                dma((2,)), dma((UNITS,)), dma,
                dma((2,)), dma((UNITS,)), dma,
                dma((2,)), dma((2,)),
            ],
            compiler_params=pltpu.CompilerParams(collective_id=0, has_side_effects=True, vmem_limit_bytes=67_000_000),
            name="stack",
        )(x, dy, w_gate, w_up, w_down)
        return outs[:4]

    tokens, weights = P(("rep", "dp"), None, None), P(None, "dp", None)
    grads = P("rep", "dp", None)
    return jax.shard_map(
        step, mesh=mesh, in_specs=(tokens, tokens, weights, weights, weights),
        out_specs=(tokens, grads, grads, grads), check_vma=False)
```

```python
import jax
import jax.numpy as jnp
from jax import lax
from jax.experimental import pallas as pl
from jax.experimental.pallas import tpu as pltpu
from jax.sharding import PartitionSpec as P

f32, bf16 = jnp.float32, jnp.bfloat16
MESH = pl.DeviceIdType.MESH
TT, D, FF, LAYERS = 2048, 512, 4096, 2
FB = 512
NF = FF // FB
UNITS = LAYERS * NF
PIECES = 3 * UNITS // 2
SLAB = 128
T = 1024
NT = TT // T
TN = 256


def dot(a, b):
    return lax.dot_general(a, b, (((1,), (0,)), ((), ())), preferred_element_type=f32)


def dot_nt(a, b):
    return lax.dot_general(a, b, (((1,), (1,)), ((), ())), preferred_element_type=f32)


def sigmoid(g):
    return 0.5 * jnp.tanh(0.5 * g) + 0.5


def tile(i, size):
    return pl.ds(pl.multiple_of(i * size, size), size)


def rms(wide):
    return lax.rsqrt(jnp.mean(wide * wide, -1, keepdims=True) + 1e-6)


def kernel(
    x_in, dy_in, wg_in, wu_in, wd_in,
    bx_out, dwg_out, dwu_out, dwd_out, WH, RDH, RXH,
    OWN, W, X, A, AT, DY, DYT, H1, ACC, PB, GB, UB, DWB, KEEP, OACC, SD, SX, RDV, RXV, OUTB,
    s_own, s_ownh, s_p, r_p, s_x, r_x, s_y, r_y, s_f, r_f, s_w, s_sd, r_rd, s_rdv, s_sx, r_rx, s_rxv, s_out, s_act,
):
    r, me = lax.axis_index("rep"), lax.axis_index("dp")
    chip, core = me // 2, me % 2
    partner = {"rep": r, "dp": chip * 2 + 1 - core}
    xnbr = {"rep": r, "dp": (1 - chip) * 2 + core}
    ynbr = {"rep": 1 - r, "dp": me}
    far = (1 - chip) * 2 + core

    def rows(d):
        return pl.ds(pl.multiple_of(d * SLAB, SLAB), SLAB)

    def remote(src, dst, send, recv, dev):
        return pltpu.make_async_remote_copy(src_ref=src, dst_ref=dst, send_sem=send, recv_sem=recv, device_id=dev, device_id_type=MESH)

    def order(j):
        return (1 - j // NF) * NF + 2 * ((j % NF) // 2) + lax.rem(r + j, 2)

    def own_loads(u):
        l, f = u // NF, u % NF
        for m, w in enumerate((wg_in, wu_in)):
            for s in range(4):
                yield pltpu.make_async_copy(
                    w.at[l, :, pl.ds(pl.multiple_of(s * 1024 + f * SLAB, SLAB), SLAB)],
                    OWN.at[u, m, :, pl.ds(s * SLAB, SLAB)], s_own.at[u])
        yield pltpu.make_async_copy(wd_in.at[l, tile(f, SLAB), :], OWN.at[u, 2], s_own.at[u])

    def own_home(u):
        return pltpu.make_async_copy(OWN.at[u], WH.at[u, :, rows(me), :], s_ownh.at[u])

    def own_partner(u):
        return remote(OWN.at[u], WH.at[u, :, rows(me), :], s_p.at[u], r_p.at[u], partner)

    def own_x(i):
        u, m = 2 * (i // 3) + r, i % 3
        return remote(OWN.at[u, m], WH.at[u, m, rows(me), :], s_x.at[i], r_x.at[i], xnbr)

    def forward_y(i):
        u, m = 2 * (i // 3) + r, i % 3
        here = WH.at[u, m, rows(far), :]
        return remote(here, here, s_y.at[i], r_y.at[i], ynbr)

    def forward_partner(u, m):
        here = WH.at[u, m, rows(far), :]
        return remote(here, here, s_f.at[u], r_f.at[u], partner)

    def forwarded(u):
        here = WH.at[u, :, rows(far), :]
        return remote(here, here, s_f.at[u], r_f.at[u], partner)

    def arrived_x(i):
        own_x(i).wait_recv()
        forward_y(i).start()
        forward_partner(2 * (i // 3) + r, i % 3).start()

    def arrived_y(i):
        forward_y(i).wait_recv()
        forward_partner(2 * (i // 3) + 1 - r, i % 3).start()

    def load_w(u, slot):
        return pltpu.make_async_copy(WH.at[u], W.at[slot], s_w.at[slot])

    def fetch_w(u, slot):
        own_partner(u).wait_recv()
        forwarded(u).wait_recv()
        load_w(u, slot).start()

    def send_terms(u, slot, m):
        return remote(SD.at[slot, m], RDH.at[u, m], s_sd.at[slot], r_rd.at[u, m], partner)

    def sent_terms(slot):
        remote(SD.at[slot], RDH.at[0], s_sd.at[slot], r_rd.at[0, 0], partner).wait_send()

    def load_terms(u, m):
        return pltpu.make_async_copy(RDH.at[u, m], RDV.at[m], s_rdv.at[m])

    def send_sum(u, slot, m):
        return remote(SX.at[slot, m], RXH.at[u, m], s_sx.at[slot], r_rx.at[u, m], xnbr)

    def sent_sum(slot):
        remote(SX.at[slot], RXH.at[0], s_sx.at[slot], r_rx.at[0, 0], xnbr).wait_send()

    def load_sum(u, m):
        return pltpu.make_async_copy(RXH.at[u, m], RXV.at[m], s_rxv.at[m])

    def store_outs(u, slot):
        l, f = u // NF, u % NF
        for m, w in enumerate((dwg_out, dwu_out)):
            for s in range(4):
                yield pltpu.make_async_copy(
                    OUTB.at[slot, m, :, pl.ds(s * SLAB, SLAB)],
                    w.at[l, :, pl.ds(pl.multiple_of(s * 1024 + f * SLAB, SLAB), SLAB)], s_out.at[slot])
        yield pltpu.make_async_copy(OUTB.at[slot, 2], dwd_out.at[l, tile(f, SLAB), :], s_out.at[slot])

    def wait_outs(slot):
        pltpu.make_async_copy(OUTB.at[slot], RXH.at[0], s_out.at[slot]).wait()

    barrier = pltpu.get_barrier_semaphore()
    for dev in (partner, xnbr, ynbr):
        pl.semaphore_signal(barrier, inc=1, device_id=dev, device_id_type=MESH)

    @pl.loop(0, UNITS)
    def _(u):
        for c in own_loads(u):
            c.start()

    load_x = pltpu.make_async_copy(x_in.at[0], X, s_act.at[0])
    load_dy = pltpu.make_async_copy(dy_in.at[0], DY, s_act.at[1])
    load_x.start()
    load_dy.start()
    pl.semaphore_wait(barrier, 3)

    @pl.loop(0, UNITS // 2)
    def _(k):
        for q in (r, 1 - r):
            u = 2 * k + q
            pltpu.make_async_copy(RXH.at[0], OWN.at[u], s_own.at[u]).wait()
            own_partner(u).start()
            own_home(u).start()
        for m in range(3):
            own_x(3 * k + m).start()

    load_x.wait()
    load_dy.wait()

    @pl.loop(0, TT // TN)
    def _(t):
        tt = tile(t, TN)
        wide = X[tt, :].astype(f32)
        A[tt, :] = (wide * rms(wide)).astype(bf16)
        DYT[:, tt] = DY[tt, :].T
        ACC[tt, :] = jnp.zeros((TN, D), f32)

    @pl.loop(0, UNITS)
    def _(u):
        own_home(u).wait()

    def forward_unit(slot):
        load_w(0, slot).wait()

        @pl.loop(0, NT)
        def _(t):
            tt = tile(t, T)
            a = A[tt, :]
            g = dot(a, W[slot, 0])
            up = dot(a, W[slot, 1])
            p = (g * sigmoid(g) * up).astype(bf16)
            ACC[tt, :] += dot(p, W[slot, 2])

    @pl.loop(0, 3 * NF // 2 + 3)
    def _(i):
        k, m = i // 3, i % 3
        arrived_x(i)

        @pl.when(i >= 2)
        def _():
            arrived_y(i - 2)

        @pl.when((i >= 3) & (m != 1))
        def _():
            @pl.when((m == 0) | (i >= 5))
            def _():
                forward_unit(m // 2)

        @pl.when(m == 2)
        def _():
            @pl.when(k < NF // 2)
            def _():
                fetch_w(2 * k + r, 0)

        @pl.when((m == 1) & (i >= 4))
        def _():
            fetch_w(2 * (k - 1) + 1 - r, 1)

    fetch_w(order(0), 0)

    @pl.loop(0, TT // TN)
    def _(t):
        tt = tile(t, TN)
        h = (X[tt, :].astype(f32) + ACC[tt, :].astype(bf16).astype(f32)).astype(bf16)
        H1[tt, :] = h
        wide = h.astype(f32)
        a = (wide * rms(wide)).astype(bf16)
        A[tt, :] = a
        AT[:, tt] = a.T
        ACC[tt, :] = jnp.zeros((TN, D), f32)

    def ask_terms(j, m):
        send_terms(order(j), 0, m).wait_recv()
        load_terms(order(j), m).start()

    def ask_sum(j, m):
        send_sum(order(j), 0, m).wait_recv()
        load_sum(order(j), m).start()

    def sum_terms(j):
        slot = j % 2

        @pl.when(j >= 2)
        def _():
            sent_sum(slot)

        for m in range(3):
            load_terms(0, m).wait()
            SX[slot, m] = (KEEP[m, 1] + RDV[m, 1].astype(f32)).astype(bf16)
            send_sum(order(j), slot, m).start()
        for m in range(3):
            OACC[j % 4, m] = KEEP[m, 0] + RDV[m, 0].astype(f32)

    def finish(j):
        slot = j % 2

        @pl.when(j >= 2)
        def _():
            wait_outs(slot)

        for m in range(3):
            load_sum(0, m).wait()
            OUTB[slot, m] = (OACC[j % 4, m] + RXV[m].astype(f32)).astype(bf16)
        for c in store_outs(order(j), slot):
            c.start()

    def hidden(t, slot):
        tt = tile(t, T)
        a = A[tt, :]
        g = dot(a, W[slot, 0])
        up = dot(a, W[slot, 1])
        dp = dot_nt(DY[tt, :], W[slot, 2]).astype(bf16).astype(f32)
        sig = sigmoid(g)
        s = g * sig
        PB[tt, :] = (s * up).astype(bf16)
        UB[tt, :] = (dp * s).astype(bf16)
        GB[tt, :] = (dp * up * (sig + s * (1 - sig))).astype(bf16)

    def to_input(t, slot):
        tt = tile(t, T)
        ACC[tt, :] += dot_nt(GB[tt, :], W[slot, 0]) + dot_nt(UB[tt, :], W[slot, 1])

    def terms(j):
        slot = j % 2

        @pl.when(j >= 2)
        def _():
            sent_terms(slot)

        for m in range(3):
            if m == 0:
                DWB[m % 2] = dot(AT[...], GB[...])
            elif m == 1:
                DWB[m % 2] = dot(AT[...], UB[...])
            else:
                DWB[m % 2] = dot(DYT[...], PB[...]).T
            SD[slot, m, 0] = DWB[m % 2, rows(partner["dp"]), :].astype(bf16)
            SD[slot, m, 1] = DWB[m % 2, rows((1 - chip) * 2 + 1 - core), :].astype(bf16)
            send_terms(order(j), slot, m).start()
            KEEP[m, 0] = DWB[m % 2, rows(me), :]
            KEEP[m, 1] = DWB[m % 2, rows(far), :]

    def ask(j):
        for m in range(3):
            ask_terms(j, m)

        @pl.when(j >= 3)
        def _():
            for m in range(3):
                ask_sum(j - 3, m)

    def take(j):
        sum_terms(j)

        @pl.when(j >= 3)
        def _():
            finish(j - 3)

    def layer_back(first, before, after):
        load_w(0, first % 3).wait()

        @pl.loop(0, NT)
        def _(t):
            hidden(t, first % 3)

        @pl.loop(first, first + NF - 1)
        def _(j):
            before(j)
            terms(j)
            load_w(0, (j + 1) % 3).wait()

            @pl.loop(0, NT)
            def _(t):
                to_input(t, j % 3)
                hidden(t, (j + 1) % 3)

                @pl.when(t == 0)
                def _():
                    ask(j)

            take(j)
            after(j)

        last = first + NF - 1
        terms(last)

        @pl.loop(0, NT)
        def _(t):
            to_input(t, last % 3)

            @pl.when(t == 0)
            def _():
                ask(last)

        take(last)

    def norm_back(h, t):
        wide = h.astype(f32)
        scale = rms(wide)
        da = ACC[tile(t, TN), :].astype(bf16).astype(f32)
        along = jnp.sum(da * wide, -1, keepdims=True) * (scale * scale * scale) * (1.0 / D)
        back = (da * scale - wide * along).astype(bf16)
        return (DY[tile(t, TN), :].astype(f32) + back.astype(f32)).astype(bf16)

    def weights_on(j):
        for m in range(3):
            @pl.when(j < 3)
            def _():
                arrived_x(15 + 3 * j + m)

            @pl.when((j >= 1) & (j < 4))
            def _():
                arrived_y(12 + 3 * j + m)

    def before_1(j):
        @pl.when(j == 0)
        def _():
            fetch_w(order(1), 1)

        @pl.when(j >= 1)
        def _():
            weights_on(j)

    def after_1(j):
        @pl.when(j < NF - 2)
        def _():
            fetch_w(order(j + 2), (j + 2) % 3)

        @pl.when(j >= NF - 2)
        def _():
            load_w(order(j + 2), (j + 2) % 3).start()

    weights_on(0)
    for i in (13, 14):
        arrived_y(i)
    layer_back(0, before_1, after_1)
    load_w(order(NF + 1), (NF + 1) % 3).start()

    @pl.loop(0, TT // TN)
    def _(t):
        tt = tile(t, TN)
        dh = norm_back(H1[tt, :], t)
        DY[tt, :] = dh
        DYT[:, tt] = dh.T
        wide = X[tt, :].astype(f32)
        a = (wide * rms(wide)).astype(bf16)
        A[tt, :] = a
        AT[:, tt] = a.T
        ACC[tt, :] = jnp.zeros((TN, D), f32)

    def after_0(j):
        @pl.when(j < UNITS - 2)
        def _():
            load_w(order(j + 2), (j + 2) % 3).start()

    layer_back(NF, lambda j: None, after_0)

    @pl.loop(0, TT // TN)
    def _(t):
        tt = tile(t, TN)
        H1[tt, :] = norm_back(X[tt, :], t)

    store_x = pltpu.make_async_copy(H1, bx_out.at[0], s_act.at[0])
    store_x.start()
    for j in range(UNITS - 3, UNITS):
        for m in range(3):
            ask_sum(j, m)
        finish(j)

    store_x.wait()
    for slot in range(2):
        wait_outs(slot)
        sent_terms(slot)
        sent_sum(slot)

    @pl.loop(0, PIECES)
    def _(i):
        own_x(i).wait_send()
        forward_y(i).wait_send()

    @pl.loop(0, UNITS)
    def _(u):
        own_partner(u).wait_send()
        forwarded(u).wait_send()


def solution(mesh):
    def step(x, dy, w_gate, w_up, w_down):
        vmem, dma = pltpu.VMEM, pltpu.SemaphoreType.DMA
        hbm = pl.BlockSpec(memory_space=pl.ANY)
        shape = jax.ShapeDtypeStruct
        outs = pl.pallas_call(
            kernel,
            out_shape=(
                shape(x.shape, bf16), shape(w_gate.shape, bf16), shape(w_up.shape, bf16), shape(w_down.shape, bf16),
                shape((UNITS, 3, D, FB), bf16), shape((UNITS, 3, 2, SLAB, FB), bf16), shape((UNITS, 3, SLAB, FB), bf16),
            ),
            in_specs=[hbm] * 5,
            out_specs=[hbm] * 7,
            scratch_shapes=[
                vmem((UNITS, 3, SLAB, FB), bf16),
                vmem((3, 3, D, FB), bf16),
                vmem((TT, D), bf16),
                vmem((TT, D), bf16),
                vmem((D, TT), bf16),
                vmem((TT, D), bf16),
                vmem((D, TT), bf16),
                vmem((TT, D), bf16),
                vmem((TT, D), f32),
                vmem((TT, FB), bf16),
                vmem((TT, FB), bf16),
                vmem((TT, FB), bf16),
                vmem((2, D, FB), f32),
                vmem((3, 2, SLAB, FB), f32),
                vmem((4, 3, SLAB, FB), f32),
                vmem((2, 3, 2, SLAB, FB), bf16),
                vmem((2, 3, SLAB, FB), bf16),
                vmem((3, 2, SLAB, FB), bf16),
                vmem((3, SLAB, FB), bf16),
                vmem((2, 3, SLAB, FB), bf16),
                dma((UNITS,)), dma((UNITS,)),
                dma((UNITS,)), dma((UNITS,)),
                dma((PIECES,)), dma((PIECES,)),
                dma((PIECES,)), dma((PIECES,)),
                dma((UNITS,)), dma((UNITS,)),
                dma((3,)),
                dma((2,)), dma((UNITS, 3)), dma((3,)),
                dma((2,)), dma((UNITS, 3)), dma((3,)),
                dma((2,)), dma((2,)),
            ],
            compiler_params=pltpu.CompilerParams(collective_id=0, has_side_effects=True, vmem_limit_bytes=67_000_000),
            name="stack",
        )(x, dy, w_gate, w_up, w_down)
        return outs[:4]

    tokens, weights = P(("rep", "dp"), None, None), P(None, "dp", None)
    grads = P("rep", "dp", None)
    return jax.shard_map(
        step, mesh=mesh, in_specs=(tokens, tokens, weights, weights, weights),
        out_specs=(tokens, grads, grads, grads), check_vma=False)
```

```python
import jax
import jax.numpy as jnp
from jax import lax
from jax.experimental import pallas as pl
from jax.experimental.pallas import tpu as pltpu
from jax.sharding import PartitionSpec as P

f32, bf16 = jnp.float32, jnp.bfloat16
MESH = pl.DeviceIdType.MESH
TT, D, FF, LAYERS = 2048, 512, 4096, 2
FB = 512
NF = FF // FB
UNITS = LAYERS * NF
PIECES = 3 * UNITS // 2
SLAB = 128
T = 1024
NT = TT // T
TN = 256


def dot(a, b):
    return lax.dot_general(a, b, (((1,), (0,)), ((), ())), preferred_element_type=f32)


def dot_nt(a, b):
    return lax.dot_general(a, b, (((1,), (1,)), ((), ())), preferred_element_type=f32)


def sigmoid(g):
    return 0.5 * jnp.tanh(0.5 * g) + 0.5


def tile(i, size):
    return pl.ds(pl.multiple_of(i * size, size), size)


def rms(wide):
    return lax.rsqrt(jnp.mean(wide * wide, -1, keepdims=True) + 1e-6)


def kernel(
    x_in, dy_in, wg_in, wu_in, wd_in,
    bx_out, dwg_out, dwu_out, dwd_out, WH, RDH, RXH, GU,
    OWN, W, X, A, AT, DY, DYT, H1, ACC, PB, GB, UB, DWB, KEEP, OACC, SD, SX, RDV, RXV, OUTB, GUV,
    s_own, s_ownh, s_p, r_p, s_x, r_x, s_y, r_y, s_f, r_f, s_w, s_sd, r_rd, s_rdv, s_sx, r_rx, s_rxv, s_out, s_act, s_gu,
):
    r, me = lax.axis_index("rep"), lax.axis_index("dp")
    chip, core = me // 2, me % 2
    partner = {"rep": r, "dp": chip * 2 + 1 - core}
    xnbr = {"rep": r, "dp": (1 - chip) * 2 + core}
    ynbr = {"rep": 1 - r, "dp": me}
    far = (1 - chip) * 2 + core

    def rows(d):
        return pl.ds(pl.multiple_of(d * SLAB, SLAB), SLAB)

    def remote(src, dst, send, recv, dev):
        return pltpu.make_async_remote_copy(src_ref=src, dst_ref=dst, send_sem=send, recv_sem=recv, device_id=dev, device_id_type=MESH)

    def order(j):
        return (1 - j // NF) * NF + 2 * ((j % NF) // 2) + lax.rem(r + j, 2)

    def own_loads(u):
        l, f = u // NF, u % NF
        for m, w in enumerate((wg_in, wu_in)):
            for s in range(4):
                yield pltpu.make_async_copy(
                    w.at[l, :, pl.ds(pl.multiple_of(s * 1024 + f * SLAB, SLAB), SLAB)],
                    OWN.at[u, m, :, pl.ds(s * SLAB, SLAB)], s_own.at[u])
        yield pltpu.make_async_copy(wd_in.at[l, tile(f, SLAB), :], OWN.at[u, 2], s_own.at[u])

    def own_home(u):
        return pltpu.make_async_copy(OWN.at[u], WH.at[u, :, rows(me), :], s_ownh.at[u])

    def own_partner(u):
        return remote(OWN.at[u], WH.at[u, :, rows(me), :], s_p.at[u], r_p.at[u], partner)

    def own_x(i):
        u, m = 2 * (i // 3) + r, i % 3
        return remote(OWN.at[u, m], WH.at[u, m, rows(me), :], s_x.at[i], r_x.at[i], xnbr)

    def forward_y(i):
        u, m = 2 * (i // 3) + r, i % 3
        here = WH.at[u, m, rows(far), :]
        return remote(here, here, s_y.at[i], r_y.at[i], ynbr)

    def forward_partner(u, m):
        here = WH.at[u, m, rows(far), :]
        return remote(here, here, s_f.at[u], r_f.at[u], partner)

    def forwarded(u):
        here = WH.at[u, :, rows(far), :]
        return remote(here, here, s_f.at[u], r_f.at[u], partner)

    def arrived_x(i):
        own_x(i).wait_recv()
        forward_y(i).start()
        forward_partner(2 * (i // 3) + r, i % 3).start()

    def arrived_y(i):
        forward_y(i).wait_recv()
        forward_partner(2 * (i // 3) + 1 - r, i % 3).start()

    def load_w(u, slot):
        return pltpu.make_async_copy(WH.at[u], W.at[slot], s_w.at[slot])

    def fetch_w(u, slot):
        own_partner(u).wait_recv()
        forwarded(u).wait_recv()
        load_w(u, slot).start()

    def send_terms(u, slot, m):
        return remote(SD.at[slot, m], RDH.at[u, m], s_sd.at[slot], r_rd.at[u, m], partner)

    def sent_terms(slot):
        remote(SD.at[slot], RDH.at[0], s_sd.at[slot], r_rd.at[0, 0], partner).wait_send()

    def load_terms(u, m):
        return pltpu.make_async_copy(RDH.at[u, m], RDV.at[m], s_rdv.at[m])

    def send_sum(u, slot, m):
        return remote(SX.at[slot, m], RXH.at[u, m], s_sx.at[slot], r_rx.at[u, m], xnbr)

    def sent_sum(slot):
        remote(SX.at[slot], RXH.at[0], s_sx.at[slot], r_rx.at[0, 0], xnbr).wait_send()

    def load_sum(u, m):
        return pltpu.make_async_copy(RXH.at[u, m], RXV.at[m], s_rxv.at[m])

    def store_outs(u, slot):
        l, f = u // NF, u % NF
        for m, w in enumerate((dwg_out, dwu_out)):
            for s in range(4):
                yield pltpu.make_async_copy(
                    OUTB.at[slot, m, :, pl.ds(s * SLAB, SLAB)],
                    w.at[l, :, pl.ds(pl.multiple_of(s * 1024 + f * SLAB, SLAB), SLAB)], s_out.at[slot])
        yield pltpu.make_async_copy(OUTB.at[slot, 2], dwd_out.at[l, tile(f, SLAB), :], s_out.at[slot])

    def wait_outs(slot):
        pltpu.make_async_copy(OUTB.at[slot], RXH.at[0], s_out.at[slot]).wait()

    barrier = pltpu.get_barrier_semaphore()
    for dev in (partner, xnbr, ynbr):
        pl.semaphore_signal(barrier, inc=1, device_id=dev, device_id_type=MESH)

    @pl.loop(0, UNITS)
    def _(u):
        for c in own_loads(u):
            c.start()

    load_x = pltpu.make_async_copy(x_in.at[0], X, s_act.at[0])
    load_dy = pltpu.make_async_copy(dy_in.at[0], DY, s_act.at[1])
    load_x.start()
    load_dy.start()
    pl.semaphore_wait(barrier, 3)

    @pl.loop(0, UNITS // 2)
    def _(k):
        for q in (r, 1 - r):
            u = 2 * k + q
            pltpu.make_async_copy(RXH.at[0], OWN.at[u], s_own.at[u]).wait()
            own_partner(u).start()
            own_home(u).start()
        for m in range(3):
            own_x(3 * k + m).start()

    load_x.wait()
    load_dy.wait()

    @pl.loop(0, TT // TN)
    def _(t):
        tt = tile(t, TN)
        wide = X[tt, :].astype(f32)
        A[tt, :] = (wide * rms(wide)).astype(bf16)
        DYT[:, tt] = DY[tt, :].T
        ACC[tt, :] = jnp.zeros((TN, D), f32)

    @pl.loop(0, UNITS)
    def _(u):
        own_home(u).wait()

    def keep_gu(u, t):
        return pltpu.make_async_copy(GUV.at[t], GU.at[u, t], s_gu.at[t])

    def load_gu(u, t):
        return pltpu.make_async_copy(GU.at[u, t], GUV.at[t], s_gu.at[t])

    def forward_unit(u, slot, again):
        load_w(0, slot).wait()

        @pl.loop(0, NT)
        def _(t):
            tt = tile(t, T)
            a = A[tt, :]
            g = dot(a, W[slot, 0])
            up = dot(a, W[slot, 1])

            @pl.when(again)
            def _():
                keep_gu(0, t).wait()

            GUV[t, 0] = g
            GUV[t, 1] = up
            p = (g * sigmoid(g) * up).astype(bf16)
            ACC[tt, :] += dot(p, W[slot, 2])
            keep_gu(u, t).start()

    @pl.loop(0, 3 * NF // 2 + 3)
    def _(i):
        k, m = i // 3, i % 3
        arrived_x(i)

        @pl.when(i >= 2)
        def _():
            arrived_y(i - 2)

        @pl.when((i >= 3) & (m != 1))
        def _():
            @pl.when((m == 0) | (i >= 5))
            def _():
                forward_unit(2 * (k - 1) + lax.rem(r + m // 2, 2), m // 2, i > 3)

        @pl.when(m == 2)
        def _():
            @pl.when(k < NF // 2)
            def _():
                fetch_w(2 * k + r, 0)

        @pl.when((m == 1) & (i >= 4))
        def _():
            fetch_w(2 * (k - 1) + 1 - r, 1)

    fetch_w(order(0), 0)
    for t in range(NT):
        keep_gu(0, t).wait()
        load_gu(order(NF), t).start()

    @pl.loop(0, TT // TN)
    def _(t):
        tt = tile(t, TN)
        h = (X[tt, :].astype(f32) + ACC[tt, :].astype(bf16).astype(f32)).astype(bf16)
        H1[tt, :] = h
        wide = h.astype(f32)
        a = (wide * rms(wide)).astype(bf16)
        A[tt, :] = a
        AT[:, tt] = a.T
        ACC[tt, :] = jnp.zeros((TN, D), f32)

    def ask_terms(j, m):
        send_terms(order(j), 0, m).wait_recv()
        load_terms(order(j), m).start()

    def ask_sum(j, m):
        send_sum(order(j), 0, m).wait_recv()
        load_sum(order(j), m).start()

    def sum_terms(j):
        slot = j % 2

        @pl.when(j >= 2)
        def _():
            sent_sum(slot)

        for m in range(3):
            load_terms(0, m).wait()
            SX[slot, m] = (KEEP[m, 1] + RDV[m, 1].astype(f32)).astype(bf16)
            send_sum(order(j), slot, m).start()
        for m in range(3):
            OACC[j % 4, m] = KEEP[m, 0] + RDV[m, 0].astype(f32)

    def finish(j):
        slot = j % 2

        @pl.when(j >= 2)
        def _():
            wait_outs(slot)

        for m in range(3):
            load_sum(0, m).wait()
            OUTB[slot, m] = (OACC[j % 4, m] + RXV[m].astype(f32)).astype(bf16)
        for c in store_outs(order(j), slot):
            c.start()

    def hidden(j, t, slot, kept):
        tt = tile(t, T)
        if kept:
            load_gu(0, t).wait()
            g, up = GUV[t, 0], GUV[t, 1]
        else:
            a = A[tt, :]
            g = dot(a, W[slot, 0])
            up = dot(a, W[slot, 1])
        dp = dot_nt(DY[tt, :], W[slot, 2]).astype(bf16).astype(f32)
        sig = sigmoid(g)
        s = g * sig
        PB[tt, :] = (s * up).astype(bf16)
        UB[tt, :] = (dp * s).astype(bf16)
        GB[tt, :] = (dp * up * (sig + s * (1 - sig))).astype(bf16)
        if kept:
            @pl.when(j < UNITS - 1)
            def _():
                load_gu(order(j + 1), t).start()

    def to_input(t, slot):
        tt = tile(t, T)
        ACC[tt, :] += dot_nt(GB[tt, :], W[slot, 0]) + dot_nt(UB[tt, :], W[slot, 1])

    def terms(j):
        slot = j % 2

        @pl.when(j >= 2)
        def _():
            sent_terms(slot)

        for m in range(3):
            if m == 0:
                DWB[m % 2] = dot(AT[...], GB[...])
            elif m == 1:
                DWB[m % 2] = dot(AT[...], UB[...])
            else:
                DWB[m % 2] = dot(DYT[...], PB[...]).T
            SD[slot, m, 0] = DWB[m % 2, rows(partner["dp"]), :].astype(bf16)
            SD[slot, m, 1] = DWB[m % 2, rows((1 - chip) * 2 + 1 - core), :].astype(bf16)
            send_terms(order(j), slot, m).start()
            KEEP[m, 0] = DWB[m % 2, rows(me), :]
            KEEP[m, 1] = DWB[m % 2, rows(far), :]

    def ask(j):
        for m in range(3):
            ask_terms(j, m)

        @pl.when(j >= 3)
        def _():
            for m in range(3):
                ask_sum(j - 3, m)

    def take(j):
        sum_terms(j)

        @pl.when(j >= 3)
        def _():
            finish(j - 3)

    def layer_back(first, kept, before, after):
        load_w(0, first % 3).wait()

        @pl.loop(0, NT)
        def _(t):
            hidden(first, t, first % 3, kept)

        @pl.loop(first, first + NF - 1)
        def _(j):
            before(j)
            terms(j)
            load_w(0, (j + 1) % 3).wait()

            @pl.loop(0, NT)
            def _(t):
                to_input(t, j % 3)
                hidden(j + 1, t, (j + 1) % 3, kept)

                @pl.when(t == 0)
                def _():
                    ask(j)

            take(j)
            after(j)

        last = first + NF - 1
        terms(last)

        @pl.loop(0, NT)
        def _(t):
            to_input(t, last % 3)

            @pl.when(t == 0)
            def _():
                ask(last)

        take(last)

    def norm_back(h, t):
        wide = h.astype(f32)
        scale = rms(wide)
        da = ACC[tile(t, TN), :].astype(bf16).astype(f32)
        along = jnp.sum(da * wide, -1, keepdims=True) * (scale * scale * scale) * (1.0 / D)
        back = (da * scale - wide * along).astype(bf16)
        return (DY[tile(t, TN), :].astype(f32) + back.astype(f32)).astype(bf16)

    def weights_on(j):
        for m in range(3):
            @pl.when(j < 3)
            def _():
                arrived_x(15 + 3 * j + m)

            @pl.when((j >= 1) & (j < 4))
            def _():
                arrived_y(12 + 3 * j + m)

    def before_1(j):
        @pl.when(j == 0)
        def _():
            fetch_w(order(1), 1)

        @pl.when(j >= 1)
        def _():
            weights_on(j)

    def after_1(j):
        @pl.when(j < NF - 2)
        def _():
            fetch_w(order(j + 2), (j + 2) % 3)

        @pl.when(j >= NF - 2)
        def _():
            load_w(order(j + 2), (j + 2) % 3).start()

    weights_on(0)
    for i in (13, 14):
        arrived_y(i)
    layer_back(0, False, before_1, after_1)
    load_w(order(NF + 1), (NF + 1) % 3).start()

    @pl.loop(0, TT // TN)
    def _(t):
        tt = tile(t, TN)
        dh = norm_back(H1[tt, :], t)
        DY[tt, :] = dh
        DYT[:, tt] = dh.T
        wide = X[tt, :].astype(f32)
        a = (wide * rms(wide)).astype(bf16)
        A[tt, :] = a
        AT[:, tt] = a.T
        ACC[tt, :] = jnp.zeros((TN, D), f32)

    def after_0(j):
        @pl.when(j < UNITS - 2)
        def _():
            load_w(order(j + 2), (j + 2) % 3).start()

    layer_back(NF, True, lambda j: None, after_0)

    @pl.loop(0, TT // TN)
    def _(t):
        tt = tile(t, TN)
        H1[tt, :] = norm_back(X[tt, :], t)

    store_x = pltpu.make_async_copy(H1, bx_out.at[0], s_act.at[0])
    store_x.start()
    for j in range(UNITS - 3, UNITS):
        for m in range(3):
            ask_sum(j, m)
        finish(j)

    store_x.wait()
    for slot in range(2):
        wait_outs(slot)
        sent_terms(slot)
        sent_sum(slot)

    @pl.loop(0, PIECES)
    def _(i):
        own_x(i).wait_send()
        forward_y(i).wait_send()

    @pl.loop(0, UNITS)
    def _(u):
        own_partner(u).wait_send()
        forwarded(u).wait_send()


def solution(mesh):
    def step(x, dy, w_gate, w_up, w_down):
        vmem, dma = pltpu.VMEM, pltpu.SemaphoreType.DMA
        hbm = pl.BlockSpec(memory_space=pl.ANY)
        shape = jax.ShapeDtypeStruct
        outs = pl.pallas_call(
            kernel,
            out_shape=(
                shape(x.shape, bf16), shape(w_gate.shape, bf16), shape(w_up.shape, bf16), shape(w_down.shape, bf16),
                shape((UNITS, 3, D, FB), bf16), shape((UNITS, 3, 2, SLAB, FB), bf16), shape((UNITS, 3, SLAB, FB), bf16),
                shape((NF, NT, 2, T, FB), f32),
            ),
            in_specs=[hbm] * 5,
            out_specs=[hbm] * 8,
            scratch_shapes=[
                vmem((UNITS, 3, SLAB, FB), bf16),
                vmem((3, 3, D, FB), bf16),
                vmem((TT, D), bf16),
                vmem((TT, D), bf16),
                vmem((D, TT), bf16),
                vmem((TT, D), bf16),
                vmem((D, TT), bf16),
                vmem((TT, D), bf16),
                vmem((TT, D), f32),
                vmem((TT, FB), bf16),
                vmem((TT, FB), bf16),
                vmem((TT, FB), bf16),
                vmem((2, D, FB), f32),
                vmem((3, 2, SLAB, FB), f32),
                vmem((4, 3, SLAB, FB), f32),
                vmem((2, 3, 2, SLAB, FB), bf16),
                vmem((2, 3, SLAB, FB), bf16),
                vmem((3, 2, SLAB, FB), bf16),
                vmem((3, SLAB, FB), bf16),
                vmem((2, 3, SLAB, FB), bf16),
                vmem((NT, 2, T, FB), f32),
                dma((UNITS,)), dma((UNITS,)),
                dma((UNITS,)), dma((UNITS,)),
                dma((PIECES,)), dma((PIECES,)),
                dma((PIECES,)), dma((PIECES,)),
                dma((UNITS,)), dma((UNITS,)),
                dma((3,)),
                dma((2,)), dma((UNITS, 3)), dma((3,)),
                dma((2,)), dma((UNITS, 3)), dma((3,)),
                dma((2,)), dma((2,)), dma((NT,)),
            ],
            compiler_params=pltpu.CompilerParams(collective_id=0, has_side_effects=True, vmem_limit_bytes=67_000_000),
            name="stack",
        )(x, dy, w_gate, w_up, w_down)
        return outs[:4]

    tokens, weights = P(("rep", "dp"), None, None), P(None, "dp", None)
    grads = P("rep", "dp", None)
    return jax.shard_map(
        step, mesh=mesh, in_specs=(tokens, tokens, weights, weights, weights),
        out_specs=(tokens, grads, grads, grads), check_vma=False)
```

```python
import jax
import jax.numpy as jnp
from jax import lax
from jax.experimental import pallas as pl
from jax.experimental.pallas import tpu as pltpu
from jax.sharding import PartitionSpec as P

f32, bf16 = jnp.float32, jnp.bfloat16
MESH = pl.DeviceIdType.MESH
TT, D, FF, LAYERS = 2048, 512, 4096, 2
FB = 512
NF = FF // FB
UNITS = LAYERS * NF
PIECES = 3 * UNITS // 2
SLAB = 128
T = 1024
NT = TT // T
TN = 256
LAG = 2


def dot(a, b):
    return lax.dot_general(a, b, (((1,), (0,)), ((), ())), preferred_element_type=f32)


def dot_nt(a, b):
    return lax.dot_general(a, b, (((1,), (1,)), ((), ())), preferred_element_type=f32)


def sigmoid(g):
    return 0.5 * jnp.tanh(0.5 * g) + 0.5


def tile(i, size):
    return pl.ds(pl.multiple_of(i * size, size), size)


def rms(wide):
    return lax.rsqrt(jnp.mean(wide * wide, -1, keepdims=True) + 1e-6)


def kernel(
    x_in, dy_in, wg_in, wu_in, wd_in,
    bx_out, dwg_out, dwu_out, dwd_out, WH, RDH, RXH, GU, AT0,
    OWN, W, X, A, AT, DY, DYT, H1, ACC, PB, GB, UB, DWB, KEEP, OACC, SD, SX, RDV, RXV, OUTB, GUV,
    s_own, s_ownh, s_p, r_p, s_x, r_x, s_y, r_y, s_f, r_f, s_w, s_sd, r_rd, s_rdv, s_sx, r_rx, s_rxv, s_out, s_act, s_gu, s_at,
):
    r, me = lax.axis_index("rep"), lax.axis_index("dp")
    chip, core = me // 2, me % 2
    partner = {"rep": r, "dp": chip * 2 + 1 - core}
    xnbr = {"rep": r, "dp": (1 - chip) * 2 + core}
    ynbr = {"rep": 1 - r, "dp": me}
    far = (1 - chip) * 2 + core

    def rows(d):
        return pl.ds(pl.multiple_of(d * SLAB, SLAB), SLAB)

    def remote(src, dst, send, recv, dev):
        return pltpu.make_async_remote_copy(src_ref=src, dst_ref=dst, send_sem=send, recv_sem=recv, device_id=dev, device_id_type=MESH)

    def order(j):
        return (1 - j // NF) * NF + 2 * ((j % NF) // 2) + lax.rem(r + j, 2)

    def own_loads(u):
        l, f = u // NF, u % NF
        for m, w in enumerate((wg_in, wu_in)):
            for s in range(4):
                yield pltpu.make_async_copy(
                    w.at[l, :, pl.ds(pl.multiple_of(s * 1024 + f * SLAB, SLAB), SLAB)],
                    OWN.at[u, m, :, pl.ds(s * SLAB, SLAB)], s_own.at[u])
        yield pltpu.make_async_copy(wd_in.at[l, tile(f, SLAB), :], OWN.at[u, 2], s_own.at[u])

    def own_home(u):
        return pltpu.make_async_copy(OWN.at[u], WH.at[u, :, rows(me), :], s_ownh.at[u])

    def own_partner(u):
        return remote(OWN.at[u], WH.at[u, :, rows(me), :], s_p.at[u], r_p.at[u], partner)

    def own_x(i):
        u, m = 2 * (i // 3) + r, i % 3
        return remote(OWN.at[u, m], WH.at[u, m, rows(me), :], s_x.at[i], r_x.at[i], xnbr)

    def forward_y(i):
        u, m = 2 * (i // 3) + r, i % 3
        here = WH.at[u, m, rows(far), :]
        return remote(here, here, s_y.at[i], r_y.at[i], ynbr)

    def forward_partner(u, m):
        here = WH.at[u, m, rows(far), :]
        return remote(here, here, s_f.at[u], r_f.at[u], partner)

    def forwarded(u):
        here = WH.at[u, :, rows(far), :]
        return remote(here, here, s_f.at[u], r_f.at[u], partner)

    def arrived_x(i):
        own_x(i).wait_recv()
        forward_y(i).start()
        forward_partner(2 * (i // 3) + r, i % 3).start()

    def arrived_y(i):
        forward_y(i).wait_recv()
        forward_partner(2 * (i // 3) + 1 - r, i % 3).start()

    def load_w(u, slot):
        return pltpu.make_async_copy(WH.at[u], W.at[slot], s_w.at[slot])

    def fetch_w(u, slot):
        own_partner(u).wait_recv()
        forwarded(u).wait_recv()
        load_w(u, slot).start()

    def send_terms(u, slot, m):
        return remote(SD.at[slot, m], RDH.at[u, m], s_sd.at[slot], r_rd.at[u, m], partner)

    def sent_terms(slot):
        remote(SD.at[slot], RDH.at[0], s_sd.at[slot], r_rd.at[0, 0], partner).wait_send()

    def load_terms(u, m):
        return pltpu.make_async_copy(RDH.at[u, m], RDV.at[m], s_rdv.at[m])

    def send_sum(u, slot, m):
        return remote(SX.at[slot, m], RXH.at[u, m], s_sx.at[slot], r_rx.at[u, m], xnbr)

    def sent_sum(slot):
        remote(SX.at[slot], RXH.at[0], s_sx.at[slot], r_rx.at[0, 0], xnbr).wait_send()

    def load_sum(u, m):
        return pltpu.make_async_copy(RXH.at[u, m], RXV.at[m], s_rxv.at[m])

    def store_outs(u, slot):
        l, f = u // NF, u % NF
        for m, w in enumerate((dwg_out, dwu_out)):
            for s in range(4):
                yield pltpu.make_async_copy(
                    OUTB.at[slot, m, :, pl.ds(s * SLAB, SLAB)],
                    w.at[l, :, pl.ds(pl.multiple_of(s * 1024 + f * SLAB, SLAB), SLAB)], s_out.at[slot])
        yield pltpu.make_async_copy(OUTB.at[slot, 2], dwd_out.at[l, tile(f, SLAB), :], s_out.at[slot])

    def wait_outs(slot):
        pltpu.make_async_copy(OUTB.at[slot], RXH.at[0], s_out.at[slot]).wait()

    barrier = pltpu.get_barrier_semaphore()
    for dev in (partner, xnbr, ynbr):
        pl.semaphore_signal(barrier, inc=1, device_id=dev, device_id_type=MESH)

    @pl.loop(0, UNITS)
    def _(u):
        for c in own_loads(u):
            c.start()

    load_x = pltpu.make_async_copy(x_in.at[0], X, s_act.at[0])
    load_dy = pltpu.make_async_copy(dy_in.at[0], DY, s_act.at[1])
    load_x.start()
    load_dy.start()
    pl.semaphore_wait(barrier, 3)

    @pl.loop(0, UNITS // 2)
    def _(k):
        for q in (r, 1 - r):
            u = 2 * k + q
            pltpu.make_async_copy(RXH.at[0], OWN.at[u], s_own.at[u]).wait()
            own_partner(u).start()
            own_home(u).start()
        for m in range(3):
            own_x(3 * k + m).start()


    def norms():
        @pl.loop(0, TT // TN)
        def _(t):
            tt = tile(t, TN)
            wide = X[tt, :].astype(f32)
            A[tt, :] = (wide * rms(wide)).astype(bf16)
            ACC[tt, :] = jnp.zeros((TN, D), f32)

    def turn(src, dst):
        @pl.loop(0, TT // TN)
        def _(t):
            tt = tile(t, TN)
            dst[:, tt] = src[tt, :].T

    park_a = pltpu.make_async_copy(AT, AT0, s_at)

    def keep_gu(u, t):
        return pltpu.make_async_copy(GUV.at[t], GU.at[u, t], s_gu.at[t])

    def load_gu(u, t):
        return pltpu.make_async_copy(GU.at[u, t], GUV.at[t], s_gu.at[t])

    def forward_unit(u, slot, again, halfway):
        load_w(0, slot).wait()

        @pl.loop(0, NT)
        def _(t):
            tt = tile(t, T)

            @pl.when(again)
            def _():
                keep_gu(0, t).wait()

            a = A[tt, :]
            g = dot(a, W[slot, 0])
            up = dot(a, W[slot, 1])
            GUV[t, 0] = g
            GUV[t, 1] = up
            p = (g * sigmoid(g) * up).astype(bf16)
            ACC[tt, :] += dot(p, W[slot, 2])
            keep_gu(u, t).start()

            @pl.when(t == 0)
            def _():
                halfway()

    @pl.loop(0, 13 + LAG)
    def _(i):
        arrived_x(i)

        @pl.when(i >= LAG)
        def _():
            arrived_y(i - LAG)

        @pl.when(i == 0)
        def _():
            load_x.wait()
            norms()

        @pl.when(i == 1)
        def _():
            load_dy.wait()
            turn(DY, DYT)

            @pl.loop(0, UNITS)
            def _(u):
                own_home(u).wait()

        @pl.when(i == 4)
        def _():
            turn(A, AT)
            park_a.start()

        b = (lax.rem(i + 3 - LAG % 3, 3) == 0) & (i >= 3 + LAG)
        a = (i % 3 == 0) & (i >= 3) & (i < 15)
        second = jnp.where(b, 1, 0)
        k = (i - 3 - LAG * second) // 3

        def next_first():
            @pl.when((i % 3 == 2) & (i < 12))
            def _():
                fetch_w(2 * (i // 3) + r, 0)

        @pl.when(a | b)
        def _():
            forward_unit(2 * k + lax.rem(r + second, 2), second, i > 3, next_first)

        @pl.when(i == 2)
        def _():
            next_first()

        @pl.when((lax.rem(i + 4 - LAG % 3, 3) == 0) & (i >= 2 + LAG))
        def _():
            fetch_w(2 * ((i - 2 - LAG) // 3) + 1 - r, 1)

    fetch_w(order(0), 0)
    park_a.wait()
    for t in range(NT):
        keep_gu(0, t).wait()
        load_gu(order(NF), t).start()

    @pl.loop(0, TT // TN)
    def _(t):
        tt = tile(t, TN)
        h = (X[tt, :].astype(f32) + ACC[tt, :].astype(bf16).astype(f32)).astype(bf16)
        H1[tt, :] = h
        wide = h.astype(f32)
        a = (wide * rms(wide)).astype(bf16)
        A[tt, :] = a
        AT[:, tt] = a.T
        ACC[tt, :] = jnp.zeros((TN, D), f32)

    def ask_terms(j, m):
        send_terms(order(j), 0, m).wait_recv()
        load_terms(order(j), m).start()

    def ask_sum(j, m):
        send_sum(order(j), 0, m).wait_recv()
        load_sum(order(j), m).start()

    def sum_piece(j, m):
        slot = j % 2
        load_terms(0, m).wait()
        SX[slot, m] = (KEEP[m, 1] + RDV[m, 1].astype(f32)).astype(bf16)
        send_sum(order(j), slot, m).start()
        OACC[j % 4, m] = KEEP[m, 0] + RDV[m, 0].astype(f32)

    def sum_terms(j):
        slot = j % 2

        @pl.when(j >= 2)
        def _():
            sent_sum(slot)

        for m in range(3):
            sum_piece(j, m)

    def finish(j):
        slot = j % 2

        @pl.when(j >= 2)
        def _():
            wait_outs(slot)

        for m in range(3):
            load_sum(0, m).wait()
            OUTB[slot, m] = (OACC[j % 4, m] + RXV[m].astype(f32)).astype(bf16)
        for c in store_outs(order(j), slot):
            c.start()

    def hidden(j, t, slot, kept):
        tt = tile(t, T)
        if kept:
            load_gu(0, t).wait()
            g, up = GUV[t, 0], GUV[t, 1]
        else:
            a = A[tt, :]
            g = dot(a, W[slot, 0])
            up = dot(a, W[slot, 1])
        dp = dot_nt(DY[tt, :], W[slot, 2]).astype(bf16).astype(f32)
        sig = sigmoid(g)
        s = g * sig
        PB[tt, :] = (s * up).astype(bf16)
        UB[tt, :] = (dp * s).astype(bf16)
        GB[tt, :] = (dp * up * (sig + s * (1 - sig))).astype(bf16)
        if kept:
            @pl.when(j < UNITS - 1)
            def _():
                load_gu(order(j + 1), t).start()

    def to_input(t, slot):
        tt = tile(t, T)
        ACC[tt, :] += dot_nt(GB[tt, :], W[slot, 0]) + dot_nt(UB[tt, :], W[slot, 1])

    def terms(j):
        slot = j % 2

        @pl.when(j >= 2)
        def _():
            sent_terms(slot)

        def cut(m):
            for q, d in enumerate((partner["dp"], (1 - chip) * 2 + 1 - core)):
                SD[slot, m, q] = DWB[m, rows(d), :].astype(bf16)
            KEEP[m, 0] = DWB[m, rows(me), :]
            KEEP[m, 1] = DWB[m, rows(far), :]

        DWB[0] = dot(AT[...], GB[...])
        DWB[1] = dot(AT[...], UB[...])
        cut(0)
        send_terms(order(j), slot, 0).start()
        DWB[2] = dot(DYT[...], PB[...]).T
        cut(1)
        send_terms(order(j), slot, 1).start()
        cut(2)
        send_terms(order(j), slot, 2).start()

    def ask(j):
        for m in range(3):
            ask_terms(j, m)

        @pl.when(j >= 3)
        def _():
            for m in range(3):
                ask_sum(j - 3, m)

    def take(j):
        sum_terms(j)

        @pl.when(j >= 3)
        def _():
            finish(j - 3)

    def layer_back(first, kept, before, after):
        load_w(0, first % 3).wait()

        @pl.loop(0, NT)
        def _(t):
            hidden(first, t, first % 3, kept)

        @pl.loop(first, first + NF - 1)
        def _(j):
            before(j)
            terms(j)
            load_w(0, (j + 1) % 3).wait()

            @pl.loop(0, NT)
            def _(t):
                to_input(t, j % 3)
                hidden(j + 1, t, (j + 1) % 3, kept)

                @pl.when(t == 0)
                def _():
                    ask(j)

            take(j)
            after(j)

        last = first + NF - 1
        terms(last)
        if not kept:
            pltpu.make_async_copy(AT0, AT, s_at).start()
        sent_sum(last % 2)
        ask_terms(last, 0)
        ask_terms(last, 1)

        @pl.loop(0, NT)
        def _(t):
            to_input(t, last % 3)

            @pl.when(t == 0)
            def _():
                sum_piece(last, 0)
                ask_terms(last, 2)
                sum_piece(last, 1)
                for m in range(3):
                    ask_sum(last - 3, m)

        sum_piece(last, 2)
        finish(last - 3)

    def norm_back(h, t):
        wide = h.astype(f32)
        scale = rms(wide)
        da = ACC[tile(t, TN), :].astype(bf16).astype(f32)
        along = jnp.sum(da * wide, -1, keepdims=True) * (scale * scale * scale) * (1.0 / D)
        back = (da * scale - wide * along).astype(bf16)
        return (DY[tile(t, TN), :].astype(f32) + back.astype(f32)).astype(bf16)

    def weights_on(j):
        for m in range(3):
            @pl.when(j < 3)
            def _():
                arrived_x(15 + 3 * j + m)

            @pl.when(j < 4)
            def _():
                arrived_y(12 + 3 * j + m)

    def before_1(j):
        @pl.when(j == 0)
        def _():
            fetch_w(order(1), 1)

        @pl.when(j >= 1)
        def _():
            weights_on(j)

    def after_1(j):
        @pl.when(j < NF - 2)
        def _():
            fetch_w(order(j + 2), (j + 2) % 3)

        @pl.when(j >= NF - 2)
        def _():
            load_w(order(j + 2), (j + 2) % 3).start()

    for i in range(13 + LAG, 18):
        arrived_x(i)
    for i in (13, 14):
        arrived_y(i)
    layer_back(0, False, before_1, after_1)
    load_w(order(NF + 1), (NF + 1) % 3).start()

    @pl.loop(0, TT // TN)
    def _(t):
        tt = tile(t, TN)
        dh = norm_back(H1[tt, :], t)
        DY[tt, :] = dh
        DYT[:, tt] = dh.T
        ACC[tt, :] = jnp.zeros((TN, D), f32)

    pltpu.make_async_copy(AT0, AT, s_at).wait()

    def after_0(j):
        @pl.when(j < UNITS - 2)
        def _():
            load_w(order(j + 2), (j + 2) % 3).start()

    layer_back(NF, True, lambda j: None, after_0)

    @pl.loop(0, TT // TN)
    def _(t):
        tt = tile(t, TN)
        H1[tt, :] = norm_back(X[tt, :], t)

    store_x = pltpu.make_async_copy(H1, bx_out.at[0], s_act.at[0])
    store_x.start()

    @pl.loop(0, PIECES)
    def _(i):
        own_x(i).wait_send()
        forward_y(i).wait_send()

    @pl.loop(0, UNITS)
    def _(u):
        own_partner(u).wait_send()
        forwarded(u).wait_send()

    for j in range(UNITS - 3, UNITS):
        for m in range(3):
            ask_sum(j, m)
        finish(j)

    store_x.wait()
    for slot in range(2):
        wait_outs(slot)
        sent_terms(slot)
        sent_sum(slot)


def solution(mesh):
    def step(x, dy, w_gate, w_up, w_down):
        vmem, dma = pltpu.VMEM, pltpu.SemaphoreType.DMA
        hbm = pl.BlockSpec(memory_space=pl.ANY)
        shape = jax.ShapeDtypeStruct
        outs = pl.pallas_call(
            kernel,
            out_shape=(
                shape(x.shape, bf16), shape(w_gate.shape, bf16), shape(w_up.shape, bf16), shape(w_down.shape, bf16),
                shape((UNITS, 3, D, FB), bf16), shape((UNITS, 3, 2, SLAB, FB), bf16), shape((UNITS, 3, SLAB, FB), bf16),
                shape((NF, NT, 2, T, FB), f32),
                shape((D, TT), bf16),
            ),
            in_specs=[hbm] * 5,
            out_specs=[hbm] * 9,
            scratch_shapes=[
                vmem((UNITS, 3, SLAB, FB), bf16),
                vmem((3, 3, D, FB), bf16),
                vmem((TT, D), bf16),
                vmem((TT, D), bf16),
                vmem((D, TT), bf16),
                vmem((TT, D), bf16),
                vmem((D, TT), bf16),
                vmem((TT, D), bf16),
                vmem((TT, D), f32),
                vmem((TT, FB), bf16),
                vmem((TT, FB), bf16),
                vmem((TT, FB), bf16),
                vmem((3, D, FB), f32),
                vmem((3, 2, SLAB, FB), f32),
                vmem((4, 3, SLAB, FB), f32),
                vmem((2, 3, 2, SLAB, FB), bf16),
                vmem((2, 3, SLAB, FB), bf16),
                vmem((3, 2, SLAB, FB), bf16),
                vmem((3, SLAB, FB), bf16),
                vmem((2, 3, SLAB, FB), bf16),
                vmem((NT, 2, T, FB), f32),
                dma((UNITS,)), dma((UNITS,)),
                dma((UNITS,)), dma((UNITS,)),
                dma((PIECES,)), dma((PIECES,)),
                dma((PIECES,)), dma((PIECES,)),
                dma((UNITS,)), dma((UNITS,)),
                dma((3,)),
                dma((2,)), dma((UNITS, 3)), dma((3,)),
                dma((2,)), dma((UNITS, 3)), dma((3,)),
                dma((2,)), dma((2,)), dma((NT,)), dma,
            ],
            compiler_params=pltpu.CompilerParams(collective_id=0, has_side_effects=True, vmem_limit_bytes=67_000_000),
            name="stack",
        )(x, dy, w_gate, w_up, w_down)
        return outs[:4]

    tokens, weights = P(("rep", "dp"), None, None), P(None, "dp", None)
    grads = P("rep", "dp", None)
    return jax.shard_map(
        step, mesh=mesh, in_specs=(tokens, tokens, weights, weights, weights),
        out_specs=(tokens, grads, grads, grads), check_vma=False)
```

```python
import jax
import jax.numpy as jnp
from jax import lax
from jax.experimental import pallas as pl
from jax.experimental.pallas import tpu as pltpu
from jax.sharding import PartitionSpec as P

f32, bf16 = jnp.float32, jnp.bfloat16
MESH = pl.DeviceIdType.MESH
TT, D, FF, LAYERS = 2048, 512, 4096, 2
FB = 512
NF = FF // FB
UNITS = LAYERS * NF
PIECES = 3 * UNITS // 2
SLAB = 128
T = 1024
NT = TT // T
TN = 256
LAG = 2


def dot(a, b):
    return lax.dot_general(a, b, (((1,), (0,)), ((), ())), preferred_element_type=f32)


def dot_nt(a, b):
    return lax.dot_general(a, b, (((1,), (1,)), ((), ())), preferred_element_type=f32)


def sigmoid(g):
    return 0.5 * jnp.tanh(0.5 * g) + 0.5


def tile(i, size):
    return pl.ds(pl.multiple_of(i * size, size), size)


def rms(wide):
    return lax.rsqrt(jnp.mean(wide * wide, -1, keepdims=True) + 1e-6)


def kernel(
    x_in, dy_in, wg_in, wu_in, wd_in,
    bx_out, dwg_out, dwu_out, dwd_out, WH, RDH, RXH, GU, AT0,
    OWN, W, X, A, AT, DY, DYT, H1, ACC, PB, GB, UB, DWB, OACC, SD, SX, RDV, RXV, OUTB, GUV,
    s_own, s_ownh, s_p, r_p, s_x, r_x, s_y, r_y, s_f, r_f, s_w, s_sd, r_rd, s_rdv, s_sx, r_rx, s_rxv, s_out, s_act, s_gu, s_at,
):
    r, me = lax.axis_index("rep"), lax.axis_index("dp")
    chip, core = me // 2, me % 2
    partner = {"rep": r, "dp": chip * 2 + 1 - core}
    xnbr = {"rep": r, "dp": (1 - chip) * 2 + core}
    ynbr = {"rep": 1 - r, "dp": me}
    far = (1 - chip) * 2 + core

    def rows(d):
        return pl.ds(pl.multiple_of(d * SLAB, SLAB), SLAB)

    def remote(src, dst, send, recv, dev):
        return pltpu.make_async_remote_copy(src_ref=src, dst_ref=dst, send_sem=send, recv_sem=recv, device_id=dev, device_id_type=MESH)

    def order(j):
        return (1 - j // NF) * NF + 2 * ((j % NF) // 2) + lax.rem(r + j, 2)

    def own_loads(u):
        l, f = u // NF, u % NF
        for m, w in enumerate((wg_in, wu_in)):
            for s in range(4):
                yield pltpu.make_async_copy(
                    w.at[l, :, pl.ds(pl.multiple_of(s * 1024 + f * SLAB, SLAB), SLAB)],
                    OWN.at[u, m, :, pl.ds(s * SLAB, SLAB)], s_own.at[u])
        yield pltpu.make_async_copy(wd_in.at[l, tile(f, SLAB), :], OWN.at[u, 2], s_own.at[u])

    def own_home(u):
        return pltpu.make_async_copy(OWN.at[u], WH.at[u, :, rows(me), :], s_ownh.at[u])

    def own_partner(u):
        return remote(OWN.at[u], WH.at[u, :, rows(me), :], s_p.at[u], r_p.at[u], partner)

    def own_x(i):
        u, m = 2 * (i // 3) + r, i % 3
        return remote(OWN.at[u, m], WH.at[u, m, rows(me), :], s_x.at[i], r_x.at[i], xnbr)

    def forward_y(i):
        u, m = 2 * (i // 3) + r, i % 3
        here = WH.at[u, m, rows(far), :]
        return remote(here, here, s_y.at[i], r_y.at[i], ynbr)

    def forward_partner(u, m):
        here = WH.at[u, m, rows(far), :]
        return remote(here, here, s_f.at[u], r_f.at[u], partner)

    def forwarded(u):
        here = WH.at[u, :, rows(far), :]
        return remote(here, here, s_f.at[u], r_f.at[u], partner)

    def arrived_x(i):
        own_x(i).wait_recv()
        forward_y(i).start()
        forward_partner(2 * (i // 3) + r, i % 3).start()

    def arrived_y(i):
        forward_y(i).wait_recv()
        forward_partner(2 * (i // 3) + 1 - r, i % 3).start()

    def load_w(u, slot):
        return pltpu.make_async_copy(WH.at[u], W.at[slot], s_w.at[slot])

    def fetch_w(u, slot):
        own_partner(u).wait_recv()
        forwarded(u).wait_recv()
        load_w(u, slot).start()

    def send_terms(u, slot, m):
        return remote(SD.at[slot, m], RDH.at[u, m], s_sd.at[slot], r_rd.at[u, m], partner)

    def sent_terms(slot):
        remote(SD.at[slot], RDH.at[0], s_sd.at[slot], r_rd.at[0, 0], partner).wait_send()

    def load_terms(u, m):
        return pltpu.make_async_copy(RDH.at[u, m], RDV.at[m], s_rdv.at[m])

    def send_sum(u, slot, m):
        return remote(SX.at[slot, m], RXH.at[u, m], s_sx.at[slot], r_rx.at[u, m], xnbr)

    def sent_sum(slot):
        remote(SX.at[slot], RXH.at[0], s_sx.at[slot], r_rx.at[0, 0], xnbr).wait_send()

    def load_sum(u, m):
        return pltpu.make_async_copy(RXH.at[u, m], RXV.at[m], s_rxv.at[m])

    def store_outs(u, slot):
        l, f = u // NF, u % NF
        for m, w in enumerate((dwg_out, dwu_out)):
            for s in range(4):
                yield pltpu.make_async_copy(
                    OUTB.at[slot, m, :, pl.ds(s * SLAB, SLAB)],
                    w.at[l, :, pl.ds(pl.multiple_of(s * 1024 + f * SLAB, SLAB), SLAB)], s_out.at[slot])
        yield pltpu.make_async_copy(OUTB.at[slot, 2], dwd_out.at[l, tile(f, SLAB), :], s_out.at[slot])

    def wait_outs(slot):
        pltpu.make_async_copy(OUTB.at[slot], RXH.at[0], s_out.at[slot]).wait()

    barrier = pltpu.get_barrier_semaphore()
    for dev in (partner, xnbr, ynbr):
        pl.semaphore_signal(barrier, inc=1, device_id=dev, device_id_type=MESH)

    @pl.loop(0, UNITS)
    def _(u):
        for c in own_loads(u):
            c.start()

    load_x = pltpu.make_async_copy(x_in.at[0], X, s_act.at[0])
    load_dy = pltpu.make_async_copy(dy_in.at[0], DY, s_act.at[1])
    load_x.start()
    load_dy.start()
    pl.semaphore_wait(barrier, 3)

    @pl.loop(0, UNITS // 2)
    def _(k):
        for q in (r, 1 - r):
            u = 2 * k + q
            pltpu.make_async_copy(RXH.at[0], OWN.at[u], s_own.at[u]).wait()
            own_partner(u).start()
            own_home(u).start()
        for m in range(3):
            own_x(3 * k + m).start()


    def norms():
        @pl.loop(0, TT // TN)
        def _(t):
            tt = tile(t, TN)
            wide = X[tt, :].astype(f32)
            A[tt, :] = (wide * rms(wide)).astype(bf16)
            ACC[tt, :] = jnp.zeros((TN, D), f32)

    def turn(src, dst):
        @pl.loop(0, TT // TN)
        def _(t):
            tt = tile(t, TN)
            dst[:, tt] = src[tt, :].T

    park_a = pltpu.make_async_copy(AT, AT0, s_at)

    def keep_gu(u, t):
        return pltpu.make_async_copy(GUV.at[t], GU.at[u, t], s_gu.at[t])

    def load_gu(u, t):
        return pltpu.make_async_copy(GU.at[u, t], GUV.at[t], s_gu.at[t])

    def forward_unit(u, slot, again, halfway):
        load_w(0, slot).wait()

        @pl.loop(0, NT)
        def _(t):
            tt = tile(t, T)

            @pl.when(again)
            def _():
                keep_gu(0, t).wait()

            a = A[tt, :]
            g = dot(a, W[slot, 0])
            up = dot(a, W[slot, 1])
            GUV[t, 0] = g
            GUV[t, 1] = up
            p = (g * sigmoid(g) * up).astype(bf16)
            ACC[tt, :] += dot(p, W[slot, 2])
            keep_gu(u, t).start()

            @pl.when(t == 0)
            def _():
                halfway()

    @pl.loop(0, 13 + LAG)
    def _(i):
        arrived_x(i)

        @pl.when(i >= LAG)
        def _():
            arrived_y(i - LAG)

        @pl.when(i == 0)
        def _():
            load_x.wait()
            norms()

        @pl.when(i == 1)
        def _():
            load_dy.wait()
            turn(DY, DYT)

            @pl.loop(0, UNITS)
            def _(u):
                own_home(u).wait()

        @pl.when(i == 4)
        def _():
            turn(A, AT)
            park_a.start()

        b = (lax.rem(i + 3 - LAG % 3, 3) == 0) & (i >= 3 + LAG)
        a = (i % 3 == 0) & (i >= 3) & (i < 15)
        second = jnp.where(b, 1, 0)
        k = (i - 3 - LAG * second) // 3

        def next_first():
            @pl.when((i % 3 == 2) & (i < 12))
            def _():
                fetch_w(2 * (i // 3) + r, 0)

        @pl.when(a | b)
        def _():
            forward_unit(2 * k + lax.rem(r + second, 2), second, i > 3, next_first)

        @pl.when(i == 2)
        def _():
            next_first()

        @pl.when((lax.rem(i + 4 - LAG % 3, 3) == 0) & (i >= 2 + LAG))
        def _():
            fetch_w(2 * ((i - 2 - LAG) // 3) + 1 - r, 1)

    fetch_w(order(0), 0)
    park_a.wait()

    @pl.loop(0, TT // TN)
    def _(t):
        tt = tile(t, TN)
        h = (X[tt, :].astype(f32) + ACC[tt, :].astype(bf16).astype(f32)).astype(bf16)
        H1[tt, :] = h
        wide = h.astype(f32)
        a = (wide * rms(wide)).astype(bf16)
        A[tt, :] = a
        AT[:, tt] = a.T
        ACC[tt, :] = jnp.zeros((TN, D), f32)

    for t in range(NT):
        keep_gu(0, t).wait()
        load_gu(order(NF), t).start()

    def ask_terms(j, m):
        send_terms(order(j), 0, m).wait_recv()
        load_terms(order(j), m).start()

    def ask_sum(j, m):
        send_sum(order(j), 0, m).wait_recv()
        load_sum(order(j), m).start()

    def sum_piece(j, m):
        slot = j % 2
        load_terms(0, m).wait()
        SX[slot, m] = (DWB[m, rows(far), :] + RDV[m, 1].astype(f32)).astype(bf16)
        send_sum(order(j), slot, m).start()
        OACC[j % 4, m] = DWB[m, rows(me), :] + RDV[m, 0].astype(f32)

    def sum_terms(j):
        slot = j % 2

        @pl.when(j >= 2)
        def _():
            sent_sum(slot)

        for m in range(3):
            sum_piece(j, m)

    def finish(j):
        slot = j % 2

        @pl.when(j >= 2)
        def _():
            wait_outs(slot)

        for m in range(3):
            load_sum(0, m).wait()
            OUTB[slot, m] = (OACC[j % 4, m] + RXV[m].astype(f32)).astype(bf16)
        for c in store_outs(order(j), slot):
            c.start()

    def hidden(j, t, slot, kept):
        tt = tile(t, T)
        if kept:
            load_gu(0, t).wait()
            g, up = GUV[t, 0], GUV[t, 1]
        else:
            a = A[tt, :]
            g = dot(a, W[slot, 0])
            up = dot(a, W[slot, 1])
        dp = dot_nt(DY[tt, :], W[slot, 2]).astype(bf16).astype(f32)
        sig = sigmoid(g)
        s = g * sig
        PB[tt, :] = (s * up).astype(bf16)
        UB[tt, :] = (dp * s).astype(bf16)
        GB[tt, :] = (dp * up * (sig + s * (1 - sig))).astype(bf16)
        if kept:
            @pl.when(j < UNITS - 1)
            def _():
                load_gu(order(j + 1), t).start()

    def to_input(t, slot):
        tt = tile(t, T)
        ACC[tt, :] += dot_nt(GB[tt, :], W[slot, 0]) + dot_nt(UB[tt, :], W[slot, 1])

    def terms(j):
        slot = j % 2

        @pl.when(j >= 2)
        def _():
            sent_terms(slot)

        def cut(m):
            for q, d in enumerate((partner["dp"], (1 - chip) * 2 + 1 - core)):
                SD[slot, m, q] = DWB[m, rows(d), :].astype(bf16)

        DWB[0] = dot(AT[...], GB[...])
        DWB[1] = dot(AT[...], UB[...])
        cut(0)
        send_terms(order(j), slot, 0).start()
        DWB[2] = dot(DYT[...], PB[...]).T
        cut(1)
        send_terms(order(j), slot, 1).start()
        cut(2)
        send_terms(order(j), slot, 2).start()

    def ask(j):
        for m in range(3):
            ask_terms(j, m)

        @pl.when(j >= 3)
        def _():
            for m in range(3):
                ask_sum(j - 3, m)

    def take(j):
        sum_terms(j)

        @pl.when(j >= 3)
        def _():
            finish(j - 3)

    def layer_back(first, kept, before, after):
        load_w(0, first % 3).wait()

        @pl.loop(0, NT)
        def _(t):
            hidden(first, t, first % 3, kept)

        @pl.loop(first, first + NF - 1)
        def _(j):
            before(j)
            terms(j)
            load_w(0, (j + 1) % 3).wait()

            if kept:
                @pl.loop(0, NT)
                def _(t):
                    to_input(t, j % 3)

                ask(j)

                @pl.loop(0, NT)
                def _(t):
                    hidden(j + 1, t, (j + 1) % 3, kept)

            else:
                @pl.loop(0, NT)
                def _(t):
                    to_input(t, j % 3)
                    hidden(j + 1, t, (j + 1) % 3, kept)

                    @pl.when(t == 0)
                    def _():
                        ask(j)

            take(j)
            after(j)

        last = first + NF - 1
        terms(last)
        if not kept:
            pltpu.make_async_copy(AT0, AT, s_at).start()
        sent_sum(last % 2)
        ask_terms(last, 0)
        ask_terms(last, 1)

        @pl.loop(0, NT)
        def _(t):
            to_input(t, last % 3)

            @pl.when(t == 0)
            def _():
                sum_piece(last, 0)
                ask_terms(last, 2)
                sum_piece(last, 1)
                for m in range(3):
                    ask_sum(last - 3, m)

        sum_piece(last, 2)
        finish(last - 3)

    def norm_back(h, t):
        wide = h.astype(f32)
        scale = rms(wide)
        da = ACC[tile(t, TN), :].astype(bf16).astype(f32)
        along = jnp.sum(da * wide, -1, keepdims=True) * (scale * scale * scale) * (1.0 / D)
        back = (da * scale - wide * along).astype(bf16)
        return (DY[tile(t, TN), :].astype(f32) + back.astype(f32)).astype(bf16)

    def weights_on(j):
        for m in range(3):
            @pl.when(j < 3)
            def _():
                arrived_x(15 + 3 * j + m)

            @pl.when(j < 4)
            def _():
                arrived_y(12 + 3 * j + m)

    def before_1(j):
        @pl.when(j == 0)
        def _():
            fetch_w(order(1), 1)

        @pl.when(j >= 1)
        def _():
            weights_on(j)

    def after_1(j):
        @pl.when(j < NF - 2)
        def _():
            fetch_w(order(j + 2), (j + 2) % 3)

        @pl.when(j >= NF - 2)
        def _():
            load_w(order(j + 2), (j + 2) % 3).start()

    for i in range(13 + LAG, 18):
        arrived_x(i)
    for i in (13, 14):
        arrived_y(i)
    layer_back(0, False, before_1, after_1)
    load_w(order(NF + 1), (NF + 1) % 3).start()

    @pl.loop(0, TT // TN)
    def _(t):
        tt = tile(t, TN)
        dh = norm_back(H1[tt, :], t)
        DY[tt, :] = dh
        DYT[:, tt] = dh.T
        ACC[tt, :] = jnp.zeros((TN, D), f32)

    pltpu.make_async_copy(AT0, AT, s_at).wait()

    def after_0(j):
        @pl.when(j < UNITS - 2)
        def _():
            load_w(order(j + 2), (j + 2) % 3).start()

    layer_back(NF, True, lambda j: None, after_0)

    @pl.loop(0, TT // TN)
    def _(t):
        tt = tile(t, TN)
        H1[tt, :] = norm_back(X[tt, :], t)

    store_x = pltpu.make_async_copy(H1, bx_out.at[0], s_act.at[0])
    store_x.start()

    @pl.loop(0, PIECES)
    def _(i):
        own_x(i).wait_send()
        forward_y(i).wait_send()

    @pl.loop(0, UNITS)
    def _(u):
        own_partner(u).wait_send()
        forwarded(u).wait_send()

    for j in range(UNITS - 3, UNITS):
        for m in range(3):
            ask_sum(j, m)
        finish(j)

    store_x.wait()
    for slot in range(2):
        wait_outs(slot)
        sent_terms(slot)
        sent_sum(slot)


CHUNKS = 4


def hand_over(*refs):
    srcs, dsts, bufs, (s_in, s_out) = refs[:4], refs[4:8], refs[8:12], refs[12:]

    def chunks():
        for q in range(CHUNKS):
            for n, src in enumerate(srcs):
                lead, size = src.shape[0], src.shape[1]
                if lead == 1:
                    yield n, q, (slice(None), pl.ds(q * (size // CHUNKS), size // CHUNKS))
                else:
                    half = size * lead // CHUNKS
                    yield n, q, (pl.ds(q * lead // CHUNKS, 1), pl.ds((q % (CHUNKS // lead)) * half, half))

    for n, q, at in chunks():
        pltpu.make_async_copy(srcs[n].at[at], bufs[n].at[at], s_in.at[n, q]).start()
    for n, q, at in chunks():
        pltpu.make_async_copy(srcs[n].at[at], bufs[n].at[at], s_in.at[n, q]).wait()
        pltpu.make_async_copy(bufs[n].at[at], dsts[n].at[at], s_out.at[n, q]).start()
    for n, q, at in chunks():
        pltpu.make_async_copy(bufs[n].at[at], dsts[n].at[at], s_out.at[n, q]).wait()


def solution(mesh):
    def step(x, dy, w_gate, w_up, w_down):
        vmem, dma = pltpu.VMEM, pltpu.SemaphoreType.DMA
        hbm = pl.BlockSpec(memory_space=pl.ANY)
        shape = jax.ShapeDtypeStruct
        outs = pl.pallas_call(
            kernel,
            out_shape=(
                shape(x.shape, bf16), shape(w_gate.shape, bf16), shape(w_up.shape, bf16), shape(w_down.shape, bf16),
                shape((UNITS, 3, D, FB), bf16), shape((UNITS, 3, 2, SLAB, FB), bf16), shape((UNITS, 3, SLAB, FB), bf16),
                shape((NF, NT, 2, T, FB), f32),
                shape((D, TT), bf16),
            ),
            in_specs=[hbm] * 5,
            out_specs=[hbm] * 9,
            scratch_shapes=[
                vmem((UNITS, 3, SLAB, FB), bf16),
                vmem((3, 3, D, FB), bf16),
                vmem((TT, D), bf16),
                vmem((TT, D), bf16),
                vmem((D, TT), bf16),
                vmem((TT, D), bf16),
                vmem((D, TT), bf16),
                vmem((TT, D), bf16),
                vmem((TT, D), f32),
                vmem((TT, FB), bf16),
                vmem((TT, FB), bf16),
                vmem((TT, FB), bf16),
                vmem((3, D, FB), f32),
                vmem((4, 3, SLAB, FB), f32),
                vmem((2, 3, 2, SLAB, FB), bf16),
                vmem((2, 3, SLAB, FB), bf16),
                vmem((3, 2, SLAB, FB), bf16),
                vmem((3, SLAB, FB), bf16),
                vmem((2, 3, SLAB, FB), bf16),
                vmem((NT, 2, T, FB), f32),
                dma((UNITS,)), dma((UNITS,)),
                dma((UNITS,)), dma((UNITS,)),
                dma((PIECES,)), dma((PIECES,)),
                dma((PIECES,)), dma((PIECES,)),
                dma((UNITS,)), dma((UNITS,)),
                dma((3,)),
                dma((2,)), dma((UNITS, 3)), dma((3,)),
                dma((2,)), dma((UNITS, 3)), dma((3,)),
                dma((2,)), dma((2,)), dma((NT,)), dma,
            ],
            compiler_params=pltpu.CompilerParams(collective_id=0, has_side_effects=True, vmem_limit_bytes=67_000_000),
            name="stack",
        )(x, dy, w_gate, w_up, w_down)
        parts = outs[:4]
        return pl.pallas_call(
            hand_over,
            out_shape=tuple(shape(p.shape, bf16) for p in parts),
            in_specs=[hbm] * 4,
            out_specs=(hbm,) * 4,
            scratch_shapes=[vmem(p.shape, bf16) for p in parts] + [dma((4, CHUNKS)), dma((4, CHUNKS))],
            name="hand_over",
        )(*parts)

    tokens, weights = P(("rep", "dp"), None, None), P(None, "dp", None)
    grads = P("rep", "dp", None)
    return jax.shard_map(
        step, mesh=mesh, in_specs=(tokens, tokens, weights, weights, weights),
        out_specs=(tokens, grads, grads, grads), check_vma=False)
```
